512 devices in a mesh: ga: 2 (over y), gx: 16 (over z), gy: 8 (over x), col: 2 (over core).
Axes of the slice: x: 8, y: 2, z: 16, core: 2. Of those that a mesh axis runs over, the one named last changes fastest.
The devices are a block of a 8x8x16 slice.
Arguments:
- pair_rep: bfloat16 [2, 640, 640, 128], P('ga', 'gx', 'gy'), parts along dimension 0, may hold values from -6 to 6
- pair_mask: int32 [2, 640, 640], P('ga', 'gx', 'gy'), parts along dimension 0, may hold values 0 or 1
- amax_history: float32 [2, 128], P(None, 'col'), may hold values from 0.3 to 3
- in_gain: float32 [128], replicated, may hold values from 0.5 to 1.5
- in_bias: float32 [128], replicated, may hold values from -3 to 3
- proj_weight: bfloat16 [128, 4, 128], P(None, None, 'col'), may hold values from -0.5 to 0.5
- gate_weight: bfloat16 [128, 128], P(None, 'col'), may hold values from -0.5 to 0.5
- out_gain: float32 [128], replicated, may hold values from 0.5 to 1.5
- out_bias: float32 [128], replicated, may hold values from -3 to 3
- out_weight: bfloat16 [128, 128], P(None, 'col'), may hold values from -0.5 to 0.5
Outputs:
- update: bfloat16 [2, 640, 640, 128], P('ga', 'gx', 'gy', 'col'), parts along dimension 0
- new_amax: float32 [4, 128], P('ga', 'col'), parts along dimension 0
The draws below stay inside these ranges and needn't reach their ends.
There are 2 independent parts, one for each index of `ga`. The reference program is written for one: setup_inputs(seed, part) draws one part's arguments, and reference() takes and returns one part's arrays. A program takes and returns all parts, laid end to end along the dimension named above; an argument that names none is the same for every part. Nothing has to cross between parts.
All inputs are finite; a program needn't handle non-finite values. No bound on the sum of `pair_mask` on one device may be relied on, other than what follows from the above.
Results may differ from the reference program's by a relative error of at most 0.0065.
Values may be sent and summed in bfloat16 or wider, within the bound.
A program may use at most 128 MiB of HBM per device.

```python
import math
import jax
import jax.numpy as jnp
from jax import lax

C = 128
CROPS = 1
N = 640


def place_ends(result, stream_key, low, top_value):
    longest = result.shape.index(max(result.shape))
    spots = []
    for shift in (0, 1):
        where = [jax.random.randint(jax.random.fold_in(stream_key, axis), (), 0, length) for axis, length in enumerate(result.shape)]
        where[longest] = (where[longest] + shift) % result.shape[longest]
        spots.append(tuple(where))
    return result.at[spots[0]].set(low).at[spots[1]].set(top_value)


def levels(key, shape, cuts, low, largest):
    level, own = 1.0, jax.random.fold_in(key, 6)
    for axis_at, blocks in cuts:
        heights = jnp.exp(jax.random.uniform(jax.random.fold_in(own, axis_at), (blocks,), jnp.float32, low / len(cuts), largest / len(cuts)))
        level = level * jnp.repeat(heights, shape[axis_at] // blocks).reshape([-1 if axis == axis_at else 1 for axis in range(len(shape))])
    return level


def scatter_about(own_key, extent, scale, reach, pieces=(), held_as=jnp.bfloat16):
    result = scale * jax.random.normal(own_key, extent, jnp.float32)
    if pieces:
        result = result * levels(own_key, extent, pieces, -0.22, 0.18)
    return jnp.clip(result, -reach, reach).astype(held_as)


def setup_inputs(seed: int = 0, part: int = 0) -> dict:
    seeds = jax.random.split(jax.random.key(seed), 11)
    part_keys = jax.random.split(jax.random.fold_in(seeds[10], part), 11)
    pair_rep = scatter_about(part_keys[0], (CROPS, N, N, C), 1.0, 6.0, ((1, 16), (2, 8)))
    pair_mask = place_ends((jax.random.randint(part_keys[1], (CROPS, N, N), 0, 10) < 9).astype(jnp.int32), jax.random.fold_in(part_keys[1], 1), 0, 1)
    amax_history = jnp.clip(jnp.exp(math.log(3.0) - 2.3025851 * jax.random.uniform(seeds[2], (2, C), jnp.float32) ** levels(seeds[2], (2, C), ((1, 2),), -0.2, 0.2)), 0.3, 3.0)
    in_gain = jnp.clip(1.0 + 0.1 * jax.random.normal(seeds[3], (C,), jnp.float32), 0.5, 1.5)
    in_bias = scatter_about(seeds[4], (C,), 0.5, 3.0, (), jnp.float32)
    proj_weight = scatter_about(seeds[5], (C, 4, C), C ** -0.5, 0.5, ((2, 2),))
    gate_weight = scatter_about(seeds[6], (C, C), C ** -0.5, 0.5, ((1, 2),))
    out_gain = jnp.clip(1.0 + 0.1 * jax.random.normal(seeds[7], (C,), jnp.float32), 0.5, 1.5)
    out_bias = scatter_about(seeds[8], (C,), 0.5, 3.0, (), jnp.float32)
    out_weight = scatter_about(seeds[9], (C, C), C ** -0.5, 0.5, ((1, 2),))
    return {"pair_rep": pair_rep, "pair_mask": pair_mask, "amax_history": amax_history, "in_gain": in_gain, "in_bias": in_bias, "proj_weight": proj_weight, "gate_weight": gate_weight, "out_gain": out_gain, "out_bias": out_bias, "out_weight": out_weight}


epsilon = 1e-05
format_limit = 448.0

def layer_norm(values, gain, bias):
    average = lax.optimization_barrier(jnp.mean(values, axis=-1, keepdims=True))
    spread = lax.optimization_barrier(jnp.mean(jnp.square(values - average), axis=-1, keepdims=True))
    return (values - average) * lax.rsqrt(spread + epsilon) * gain + bias

def one_crop(crop_rep, crop_mask, amax_history, in_gain, in_bias, proj_weight, gate_weight, out_gain, out_bias, out_weight):
    normed = layer_norm(crop_rep.astype(jnp.float32), in_gain, in_bias).astype(jnp.bfloat16)
    flat = normed.reshape(N * N, C)
    masking = crop_mask.astype(jnp.float32).reshape(N * N, 1)

    def project(which):
        return jnp.dot(flat, proj_weight[:, which, :], preferred_element_type=jnp.float32)
    left_proj = masking * jax.nn.sigmoid(project(1)) * project(0)
    right_proj = masking * jax.nn.sigmoid(project(3)) * project(2)
    crop_amax = jnp.stack([lax.optimization_barrier(jnp.max(jnp.abs(left_proj), axis=0)), lax.optimization_barrier(jnp.max(jnp.abs(right_proj), axis=0))])
    scales = amax_history / format_limit
    left_q = jnp.clip(left_proj / scales[0], -format_limit, format_limit).astype(jnp.bfloat16).reshape(N, N, C)
    right_q = jnp.clip(right_proj / scales[1], -format_limit, format_limit).astype(jnp.bfloat16).reshape(N, N, C)
    products = jnp.einsum('ikc,jkc->ijc', left_q.astype(jnp.float32), right_q.astype(jnp.float32))
    triangle = (products * (scales[0] * scales[1])).astype(jnp.bfloat16)
    tnorm = layer_norm(triangle.astype(jnp.float32), out_gain, out_bias).astype(jnp.bfloat16)
    gating = jax.nn.sigmoid(jnp.dot(flat, gate_weight, preferred_element_type=jnp.float32))
    mixing = jnp.dot(tnorm.reshape(N * N, C), out_weight, preferred_element_type=jnp.float32)
    update = (gating * mixing).astype(jnp.bfloat16).reshape(N, N, C)
    return (update, crop_amax)

def reference(pair_rep, pair_mask, amax_history, in_gain, in_bias, proj_weight, gate_weight, out_gain, out_bias, out_weight):
    updates = []
    maxima = []
    for crop in range(CROPS):
        update, crop_amax = one_crop(pair_rep[crop], pair_mask[crop], amax_history, in_gain, in_bias, proj_weight, gate_weight, out_gain, out_bias, out_weight)
        updates.append(update)
        maxima.append(crop_amax)
    new_amax = maxima[0]
    for crop_amax in maxima[1:]:
        new_amax = jnp.maximum(new_amax, crop_amax)
    return (jnp.stack(updates), new_amax)
```

```python
import functools

import jax
import jax.numpy as jnp
from jax import lax
from jax.experimental import pallas as pl
from jax.experimental.pallas import tpu as pltpu
from jax.sharding import PartitionSpec as P

epsilon = 1e-05
format_limit = 448.0
MESH = pl.DeviceIdType.MESH
f32, bf16 = jnp.float32, jnp.bfloat16


def block_transpose(parts):
    parts = list(parts)
    shape = parts[0].shape
    block = lax.broadcasted_iota(jnp.int32, shape, len(shape) - 1) // 16
    for bit in (4, 2, 1):
        low = (block & bit) == 0
        for a in range(8):
            if a & bit:
                continue
            x, y = parts[a], parts[a | bit]
            parts[a] = jnp.where(low, x, pltpu.roll(y, 16 * bit, 1))
            parts[a | bit] = jnp.where(low, pltpu.roll(x, 128 - 16 * bit, 1), y)
    return parts


def kernel(
    sizes,
    pair_ref,
    mask_ref,
    w_ref,
    inv_ref,
    back_ref,
    gain_ref,
    bias_ref,
    gate_w_ref,
    out_gain_ref,
    out_bias_ref,
    out_w_ref,
    out_ref,
    amax_ref,
    normed,
    gates,
    peak,
    xsend,
    xrecv,
    staged,
    ready,
    rhome,
    rmat,
    lhome,
    tsend,
    trecv,
    staged2,
    txsend,
    tfull,
    peak_x,
    peak_z,
    x_ss,
    x_rs,
    r_ss,
    r_rs,
    l_ss,
    l_rs,
    t_ss,
    t_rs,
    tx_ss,
    tx_rs,
    d_ss,
    d_rs,
    px_ss,
    px_rs,
    pz_ss,
    pz_rs,
):
    nz, nx, chunks = sizes
    z, x, core = lax.axis_index("gx"), lax.axis_index("gy"), lax.axis_index("col")
    other = 1 - core
    half = nz // 2

    def zp(d):
        return lax.rem(z + d, nz)

    def xp(d):
        return lax.rem(x + d, nx)

    sends = []

    def send(src, dst, ss, rs, target):
        copy = pltpu.make_async_remote_copy(
            src_ref=src,
            dst_ref=dst,
            send_sem=ss,
            recv_sem=rs,
            device_id=target,
            device_id_type=MESH,
        )
        copy.start()
        sends.append(copy)

    def arrived(dst, rs):
        pltpu.make_async_copy(dst, dst, rs).wait()

    barrier = pltpu.get_barrier_semaphore()
    for d in range(1, nx):
        pl.semaphore_signal(barrier, inc=1, device_id={"gy": xp(d)}, device_id_type=MESH)
    for d in range(1, nz):
        pl.semaphore_signal(barrier, inc=1, device_id={"gx": zp(d)}, device_id_type=MESH)
    pl.semaphore_signal(barrier, inc=1, device_id={"col": other}, device_id_type=MESH)

    far = nz // 4
    z_order = []
    for d in range(nz // 2, 0, -1):
        z_order.append(d)
        if nz - d != d:
            z_order.append(nz - d)
    x_order = []
    for d in range(nx // 2, 0, -1):
        x_order.append(d)
        if nx - d != d:
            x_order.append(nx - d)
    arc = [e % nz for e in range(1 - far, far)] + [lax.rem(far + half * core, nz)]
    own = far - 1

    for c in range(chunks):
        rows = pair_ref[8 * c : 8 * c + 8].reshape(640, 128).astype(f32)
        average = jnp.mean(rows, axis=-1, keepdims=True)
        centred = rows - average
        spread = jnp.mean(centred * centred, axis=-1, keepdims=True)
        flat = (centred * lax.rsqrt(spread + epsilon) * gain_ref[...] + bias_ref[...]).astype(bf16)
        normed[640 * c : 640 * c + 640, :] = flat
        proj = lax.dot_general(
            w_ref[...], flat, (((1,), (1,)), ((), ())), preferred_element_type=f32
        )
        both = mask_ref[c] * jax.nn.sigmoid(proj[128:]) * proj[:128]
        top = jnp.abs(both)
        top = jnp.maximum(
            jnp.maximum(
                jnp.maximum(top[:, :128], top[:, 128:256]),
                jnp.maximum(top[:, 256:384], top[:, 384:512]),
            ),
            top[:, 512:],
        )
        peak[...] = top if c == 0 else jnp.maximum(peak[...], top)
        quant = jnp.clip(both * inv_ref[...], -format_limit, format_limit).astype(bf16)
        xsend[c] = quant.reshape(8, 16, 640)
        xrecv[c, x] = xsend[c, x]
        if c == 0:
            pl.semaphore_wait(barrier, nx + nz - 1)
        for d in x_order:
            t = xp(d)
            send(xsend.at[c, t], xrecv.at[c, x], x_ss.at[c, d], x_rs.at[c, d], {"gy": t})

    for c in range(chunks):
        for d in x_order:
            arrived(xrecv.at[c, xp(nx - d)], x_rs.at[c, d])
        for g in range(5):
            parts = [xrecv[c, a, :, 128 * g : 128 * g + 128].astype(f32) for a in range(8)]
            for p, part in enumerate(block_transpose(parts)):
                staged[16 * (8 * g + p) : 16 * (8 * g + p) + 16, :] = part
        for r in range(16):
            tiles = [staged[pl.ds(16 * k + r, 8, stride=80), :] for k in range(5)]
            ready[r, c] = jnp.concatenate(tiles, axis=1).astype(bf16)
        rhome[c, z] = ready[8 + lax.rem(z, half), c]
        for d in z_order:
            t = zp(d)
            send(
                ready.at[8 + lax.rem(t, half), c],
                rhome.at[c, z],
                r_ss.at[c, d],
                r_rs.at[c, d],
                {"gx": t},
            )

    for c in range(chunks):
        for a, e in enumerate(arc):
            if a == own:
                lhome[c, a] = ready[lax.rem(z, half), c]
                continue
            t = zp(e)
            send(
                ready.at[lax.rem(t, half), c],
                lhome.at[c, a],
                l_ss.at[c, a],
                l_rs.at[c, a],
                {"gx": t},
            )

    tops = peak[...].reshape(8, 2, 8, 128)
    tops = jnp.concatenate([tops[:, 0].reshape(64, 128), tops[:, 1].reshape(64, 128)], axis=0)
    peak_x[x] = jnp.max(tops.T, axis=0, keepdims=True)
    for d in x_order:
        send(peak_x.at[x], peak_x.at[x], px_ss.at[d], px_rs.at[d], {"gy": xp(d)})
    for c in range(chunks):
        gates[640 * c : 640 * c + 640, :] = jax.nn.sigmoid(
            jnp.dot(normed[640 * c : 640 * c + 640, :], gate_w_ref[...], preferred_element_type=f32)
        )
    for d in x_order:
        arrived(peak_x.at[xp(nx - d)], px_rs.at[d])
    peak_z[z] = jnp.max(peak_x[...], axis=0)
    for d in z_order:
        send(peak_z.at[z], peak_z.at[z], pz_ss.at[d], pz_rs.at[d], {"gx": zp(d)})

    for c in range(chunks):
        for d in z_order:
            arrived(rhome.at[c, zp(nz - d)], r_rs.at[c, d])
        rmat[128 * c : 128 * c + 128, :] = rhome[c].astype(f32).reshape(128, 640).astype(bf16)

    for c in range(chunks):
        for a in range(len(arc)):
            if a != own:
                arrived(lhome.at[c, a], l_rs.at[c, a])
        left = lhome[c].astype(f32).reshape(64, 640).astype(bf16)
        product = lax.dot_general(
            left, rmat[...], (((1,), (1,)), ((), ())), preferred_element_type=f32
        )
        scaled = product * back_ref[x, lax.rem(z, half)]
        tsend[c] = scaled.reshape(8, 8, 640).astype(bf16)
        for a, e in enumerate(arc):
            if a == own:
                trecv[c, lax.rem(z, half)] = tsend[c, a]
                continue
            t = zp(nz - e)
            send(
                tsend.at[c, a],
                trecv.at[c, lax.rem(z, half)],
                t_ss.at[c, a],
                t_rs.at[c, a],
                {"gx": t},
            )

    def over_x(c):
        for a, e in enumerate(arc):
            if a != own:
                arrived(trecv.at[c, lax.rem(zp(e), half)], t_rs.at[c, a])
        for s in range(8):
            for j in range(5):
                staged2[pl.ds(8 * j + s, 8, stride=40), :] = trecv[
                    c, s, :, 128 * j : 128 * j + 128
                ].astype(f32)
        for g in range(5):
            parts = [staged2[8 * (8 * g + p) : 8 * (8 * g + p) + 8, :] for p in range(8)]
            for b, part in enumerate(block_transpose(parts)):
                txsend[c, b, :, 128 * g : 128 * g + 128] = part.astype(bf16)
        tfull[c, core, x] = txsend[c, x]
        for d in x_order:
            t = xp(d)
            send(txsend.at[c, t], tfull.at[c, core, x], tx_ss.at[c, d], tx_rs.at[c, d], {"gy": t})

    def over_core(c):
        for d in x_order:
            arrived(tfull.at[c, core, xp(nx - d)], tx_rs.at[c, d])
        send(tfull.at[c, core], tfull.at[c, core], d_ss.at[c], d_rs.at[c], {"col": other})

    def finish(c):
        arrived(tfull.at[c, other], d_rs.at[c])
        values = tfull[c].astype(f32).reshape(128, 640)
        average = jnp.mean(values, axis=0, keepdims=True)
        centred = values - average
        spread = jnp.mean(centred * centred, axis=0, keepdims=True)
        tnorm = (
            centred * lax.rsqrt(spread + epsilon) * out_gain_ref[...] + out_bias_ref[...]
        ).astype(bf16)
        mixing = lax.dot_general(
            tnorm, out_w_ref[...], (((0,), (0,)), ((), ())), preferred_element_type=f32
        )
        groups = mixing.reshape(8, 5, 2, 8, 64)
        gate = gates[640 * c : 640 * c + 640, :].reshape(8, 2, 5, 8, 64)
        for b in range(2):
            for j in range(5):
                out_ref[8 * c : 8 * c + 8, 40 * b + 8 * j : 40 * b + 8 * j + 8, :] = (
                    gate[:, b, j] * groups[:, j, b]
                ).astype(bf16)

    for step in range(chunks + 2):
        if step < chunks:
            over_x(step)
        if 0 <= step - 1 < chunks:
            over_core(step - 1)
        if 0 <= step - 2 < chunks:
            finish(step - 2)

    for d in z_order:
        arrived(peak_z.at[zp(nz - d)], pz_rs.at[d])
    tops = jnp.max(peak_z[...], axis=0)
    amax_ref[0:1, :] = tops[:, :64]
    amax_ref[1:2, :] = tops[:, 64:]

    for copy in sends:
        copy.wait_send()


def solution(mesh):
    nz, nx = mesh.shape["gx"], mesh.shape["gy"]

    def on_device(
        pair_rep,
        pair_mask,
        amax_history,
        in_gain,
        in_bias,
        proj_weight,
        gate_weight,
        out_gain,
        out_bias,
        out_weight,
    ):
        _, ni, nj, width = pair_rep.shape
        held = proj_weight.shape[2]
        chunks = ni // 8
        assert nx == 8 and nz == 16 and nj == 80 and width == 128 and held == 64
        lanes = 8 * nj
        ordered = proj_weight.transpose(1, 2, 0).reshape(2, 2, nx, 8, width)
        weights = ordered.transpose(1, 2, 0, 3, 4).reshape(4 * held, width)
        scales = amax_history / format_limit
        inverse = (1.0 / scales).reshape(2, nx, 8).transpose(1, 0, 2).reshape(2 * held, 1)
        back = (scales[0] * scales[1]).reshape(nx, 8, 1, 1)
        masking = pair_mask.astype(f32).reshape(chunks, 1, lanes)
        vmem = pl.BlockSpec(memory_space=pltpu.VMEM)
        dma = pltpu.SemaphoreType.DMA
        update, amax = pl.pallas_call(
            functools.partial(kernel, (nz, nx, chunks)),
            out_shape=(
                jax.ShapeDtypeStruct((ni, nj, held), bf16),
                jax.ShapeDtypeStruct((2, held), f32),
            ),
            in_specs=[vmem] * 11,
            out_specs=(vmem, vmem),
            scratch_shapes=[
                pltpu.VMEM((ni * nj, width), bf16),
                pltpu.VMEM((ni * nj, held), f32),
                pltpu.VMEM((2 * held, 128), f32),
                pltpu.VMEM((chunks, nx, 16, lanes), bf16),
                pltpu.VMEM((chunks, nx, 16, lanes), bf16),
                pltpu.VMEM((16 * 40, 128), f32),
                pltpu.VMEM((16, chunks, 8, lanes), bf16),
                pltpu.VMEM((chunks, nz, 8, lanes), bf16),
                pltpu.VMEM((chunks * 128, lanes), bf16),
                pltpu.VMEM((chunks, 8, 8, lanes), bf16),
                pltpu.VMEM((chunks, 8, 8, lanes), bf16),
                pltpu.VMEM((chunks, 8, 8, lanes), bf16),
                pltpu.VMEM((8 * 40, 128), f32),
                pltpu.VMEM((chunks, nx, 8, lanes), bf16),
                pltpu.VMEM((chunks, 2, nx, 8, lanes), bf16),
                pltpu.VMEM((nx, 1, 128), f32),
                pltpu.VMEM((nz, 1, 128), f32),
                dma((chunks, nx)),
                dma((chunks, nx)),
                dma((chunks, nz)),
                dma((chunks, nz)),
                dma((chunks, 8)),
                dma((chunks, 8)),
                dma((chunks, 8)),
                dma((chunks, 8)),
                dma((chunks, nx)),
                dma((chunks, nx)),
                dma((chunks,)),
                dma((chunks,)),
                dma((nx,)),
                dma((nx,)),
                dma((nz,)),
                dma((nz,)),
            ],
            compiler_params=pltpu.CompilerParams(
                collective_id=0, has_side_effects=True, vmem_limit_bytes=48 * 2**20
            ),
            name="triangle",
        )(
            pair_rep[0],
            masking,
            weights,
            inverse,
            back,
            in_gain[None],
            in_bias[None],
            gate_weight,
            out_gain[:, None],
            out_bias[:, None],
            out_weight,
        )
        return update[None], amax

    placed = (
        P("ga", "gx", "gy", None),
        P("ga", "gx", "gy"),
        P(None, "col"),
        P(),
        P(),
        P(None, None, "col"),
        P(None, "col"),
        P(),
        P(),
        P(None, "col"),
    )
    return jax.shard_map(
        on_device,
        mesh=mesh,
        in_specs=placed,
        out_specs=(P("ga", "gx", "gy", "col"), P("ga", "col")),
        check_vma=False,
    )
```

```python
import functools

import jax
import jax.numpy as jnp
from jax import lax
from jax.experimental import pallas as pl
from jax.experimental.pallas import tpu as pltpu
from jax.sharding import PartitionSpec as P

epsilon = 1e-05
format_limit = 448.0
MESH = pl.DeviceIdType.MESH
f32, bf16 = jnp.float32, jnp.bfloat16


def block_transpose(parts):
    parts = list(parts)
    shape = parts[0].shape
    block = lax.broadcasted_iota(jnp.int32, shape, len(shape) - 1) // 16
    for bit in (4, 2, 1):
        low = (block & bit) == 0
        for a in range(8):
            if a & bit:
                continue
            x, y = parts[a], parts[a | bit]
            parts[a] = jnp.where(low, x, pltpu.roll(y, 16 * bit, 1))
            parts[a | bit] = jnp.where(low, pltpu.roll(x, 128 - 16 * bit, 1), y)
    return parts


def kernel(sizes, *refs):
    nz, nx, chunks, names = sizes
    ref = dict(zip(names, refs))
    z, x, core = lax.axis_index("gx"), lax.axis_index("gy"), lax.axis_index("col")
    other = 1 - core
    half = nz // 2
    slot = lax.rem(z, half)
    lanes = 640

    def column(row, width):
        return jnp.broadcast_to(row, (width, row.shape[1])).T

    def load(name):
        return pltpu.make_async_copy(ref[name + "_h"], ref[name], ref["in_sem"].at[inputs.index(name)])

    inputs = [n[:-2] for n in names if n.endswith("_h") and n != "pair_h"]

    def pair_load(c):
        return pltpu.make_async_copy(
            ref["pair_h"].at[0, pl.ds(8 * c, 8)], ref["pair"].at[pl.ds(8 * c, 8)], ref["pair_sem"].at[c]
        )

    def send(src, dst, ss, rs, target):
        pltpu.make_async_remote_copy(
            src_ref=src, dst_ref=dst, send_sem=ss, recv_sem=rs, device_id=target, device_id_type=MESH
        ).start()

    def await_bytes(like, sem):
        pltpu.make_async_copy(like, like, sem).wait()

    def zp(d):
        return lax.rem(z + d, nz)

    def xp(d):
        return lax.rem(x + d, nx)

    rank = lax.rem(z + nz - 1, nz)

    def ranked(r):
        return lax.rem(r + 1, nz)

    def each(low, high, body):
        def step(i, carry):
            body(i)
            return carry

        lax.fori_loop(low, high, step, 0)

    barrier = pltpu.get_barrier_semaphore()
    for d in range(1, nx):
        pl.semaphore_signal(barrier, inc=1, device_id={"gy": xp(d)}, device_id_type=MESH)
    pl.semaphore_signal(barrier, inc=1, device_id={"col": other}, device_id_type=MESH)
    each(
        rank + 1,
        nz,
        lambda r: pl.semaphore_signal(
            barrier, inc=1, device_id={"gx": ranked(r)}, device_id_type=MESH
        ),
    )
    for name in inputs[:6]:
        load(name).start()
    for c in range(chunks):
        pair_load(c).start()
    for name in inputs[6:]:
        load(name).start()
    with jax.named_scope("input"):
        for name in inputs:
            load(name).wait()

    x_order = []
    for d in range(nx // 2, 0, -1):
        x_order.append(d)
        if nx - d != d:
            x_order.append(nx - d)

    def x_send(kind, c):
        for d in x_order:
            t = xp(d)
            send(
                ref["xs" + kind].at[c, t],
                ref["xr" + kind].at[c, x],
                ref[f"xs{kind}_ss"].at[0],
                ref[f"xs{kind}_rs"].at[c],
                {"gy": t},
            )

    history = ref["history"][...]
    inverse = format_limit / history
    inverse_left = column(inverse[0:1, :], 128)
    inverse_right = column(inverse[1:2, :], 128)
    weights = ref["w"][...].reshape(256, 128)
    for c in range(chunks):
        with jax.named_scope("pair"):
            pair_load(c).wait()
        with jax.named_scope("norm"):
            rows = ref["pair"][8 * c : 8 * c + 8].reshape(lanes, 128).astype(f32)
            average = jnp.mean(rows, axis=-1, keepdims=True)
            centred = rows - average
            spread = jnp.mean(centred * centred, axis=-1, keepdims=True)
            flat = (
                centred * lax.rsqrt(spread + epsilon) * ref["gain"][...] + ref["bias"][...]
            ).astype(bf16)
            ref["normed"][lanes * c : lanes * c + lanes, :] = flat
            kept = ref["mask"][0, 8 * c : 8 * c + 8, :].astype(f32).T
            masked = jnp.concatenate(
                [flat[80 * i : 80 * i + 80] * kept[:, i : i + 1].astype(bf16) for i in range(8)], axis=0
            )
            proj = lax.dot_general(
                weights, masked, (((1,), (1,)), ((), ())), preferred_element_type=f32
            )
        with jax.named_scope("quant"):
            for kind, base, inv in (("r", 128, inverse_right), ("l", 0, inverse_left)):
                both = jax.nn.sigmoid(proj[base + 64 : base + 128]) * proj[base : base + 64]
                tiles = [both[:, 128 * k : 128 * k + 128] for k in range(5)]
                top = functools.reduce(jnp.maximum, [jnp.abs(tile) for tile in tiles])
                peak = ref["peak" + kind]
                peak[...] = top if c == 0 else jnp.maximum(peak[...], top)
                quant = jnp.concatenate(
                    [jnp.clip(tile * inv, -format_limit, format_limit) for tile in tiles], axis=1
                )
                ref["xs" + kind][c] = quant.astype(bf16).reshape(8, 8, lanes)
                ref["xr" + kind][c, x] = ref["xs" + kind][c, x]
                if kind == "r":
                    if c == 0:
                        with jax.named_scope("entry"):
                            pl.semaphore_wait(barrier, nx + rank)
                        each(
                            0,
                            rank,
                            lambda r: pl.semaphore_signal(
                                ref["known"].at[z], inc=1, device_id={"gx": ranked(r)}, device_id_type=MESH
                            ),
                        )
                    x_send("r", c)
    for c in range(chunks):
        x_send("l", c)
    with jax.named_scope("peak"):
        tops = jnp.concatenate([ref["peakl"][...], ref["peakr"][...]], axis=0)
        ref["peak_x"][x] = jnp.max(tops.T, axis=0, keepdims=True)
        for d in x_order:
            send(
                ref["peak_x"].at[x],
                ref["peak_x"].at[x],
                ref["px_ss"].at[0],
                ref["px_rs"].at[0],
                {"gy": xp(d)},
            )
    with jax.named_scope("gate"):
        for c in range(chunks):
            ref["gates"][c] = jax.nn.sigmoid(
                lax.dot_general(
                    ref["gate_w"][...],
                    ref["normed"][lanes * c : lanes * c + lanes, :],
                    (((1,), (1,)), ((), ())),
                    preferred_element_type=f32,
                )
            )

    def gather_rows(kind, c):
        with jax.named_scope("xwait" + kind):
            await_bytes(ref["xr" + kind].at[c, pl.ds(0, nx - 1)], ref[f"xs{kind}_rs"].at[c])
        staged = ref["staged"]
        with jax.named_scope("relay" + kind):
            for g in range(5):
                parts = [
                    ref["xr" + kind][c, a, :, 128 * g : 128 * g + 128].astype(f32) for a in range(8)
                ]
                for p, part in enumerate(block_transpose(parts)):
                    staged[8 * (8 * g + p) : 8 * (8 * g + p) + 8, :] = part
            for s in range(8):
                tiles = [staged[pl.ds(8 * k + s, 8, stride=40), :] for k in range(5)]
                ref["ready" + kind][s, c] = jnp.concatenate(tiles, axis=1).astype(bf16)

    def send_right(c, t):
        send(
            ref["readyr"].at[lax.rem(t, half), c],
            ref["rhome"].at[z, c],
            ref["r_ss"].at[0],
            ref["r_rs"].at[z],
            {"gx": t},
        )

    def send_left(c, t):
        send(
            ref["readyl"].at[lax.rem(t, half), c],
            ref["lhome"].at[slot, c],
            ref["l_ss"].at[0],
            ref["l_rs"].at[slot],
            {"gx": t},
        )

    def in_arc(t):
        e = lax.rem(t - z + nz, nz)
        return (e < half // 2) | (e > nz - half // 2) | (e == half // 2 + half * core)

    def send_peak(t):
        send(
            ref["peak_z"].at[z], ref["peak_z"].at[z], ref["pz_ss"].at[0], ref["pz_rs"].at[0], {"gx": t}
        )

    ahead = half // 2
    near = lax.min(rank + 1 + ahead, nz)

    def left_to(r):
        t = ranked(r)

        @pl.when(in_arc(t))
        def _():
            for c in range(chunks):
                send_left(c, t)

    def right_to(r):
        t = ranked(r)
        pl.semaphore_wait(ref["known"].at[t], 1)
        for c in range(chunks):
            send_right(c, t)

    def rest_to(r):
        right_to(r)
        left_to(r)
        send_peak(ranked(r))

    for c in range(chunks):
        gather_rows("r", c)
        ref["rhome"][z, c] = ref["readyr"][slot, c]
        each(0, rank, lambda r: send_right(c, ranked(r)))
    with jax.named_scope("near"):
        each(rank + 1, near, right_to)
    for c in range(chunks):
        gather_rows("l", c)
        ref["lhome"][slot, c] = ref["readyl"][slot, c]

        def left_below(r):
            t = ranked(r)

            @pl.when(in_arc(t))
            def _():
                send_left(c, t)

        each(0, rank, left_below)
    each(rank + 1, near, left_to)
    with jax.named_scope("peakwait"):
        await_bytes(ref["peak_x"].at[pl.ds(0, nx - 1)], ref["px_rs"].at[0])
    ref["peak_z"][z] = jnp.max(ref["peak_x"][...], axis=0)
    each(0, rank, lambda r: send_peak(ranked(r)))
    each(rank + 1, near, lambda r: send_peak(ranked(r)))
    with jax.named_scope("higher"):
        each(near, nz, rest_to)
    with jax.named_scope("sentx"):
        await_bytes(ref["peak_x"].at[pl.ds(0, nx - 1)], ref["px_ss"].at[0])
        await_bytes(ref["lhome"].at[pl.ds(0, nx - 1)], ref["xsr_ss"].at[0])
        await_bytes(ref["lhome"].at[pl.ds(0, nx - 1)], ref["xsl_ss"].at[0])

    def right_arrived(n):
        source = zp(n)
        await_bytes(ref["rhome"].at[source], ref["r_rs"].at[source])

    with jax.named_scope("rightwait"):
        each(1, nz, right_arrived)
    with jax.named_scope("rmat"):
        for t in range(5):
            granules = []
            for b in range(8):
                for g in (2 * t, 2 * t + 1):
                    granules.append(ref["rhome"][2 * b + g // 5, g % 5].astype(f32))
            ref["rmat"][128 * t : 128 * t + 128, :] = jnp.concatenate(granules, axis=0).astype(bf16)

    product_scale = history[0:1, :] * history[1:2, :] * (1.0 / format_limit / format_limit)
    channel = 8 * x + slot
    here = lax.broadcasted_iota(jnp.int32, product_scale.shape, 1) == channel
    back = jnp.sum(jnp.where(here, product_scale, 0.0), axis=1, keepdims=True)
    first = lax.rem(rank - half // 2 + core + nz, nz)
    turn = jnp.where(first > half, nz - first, 0)

    def triangle(n):
        row = ranked(lax.rem(first + lax.rem(turn + n, half), nz))
        place = lax.rem(row, half)

        with jax.named_scope("leftwait"):
            @pl.when(row != z)
            def _():
                await_bytes(ref["lhome"].at[place], ref["l_rs"].at[place])

        with jax.named_scope("dot"):
            left = ref["lhome"][place].astype(f32).reshape(40, lanes).astype(bf16)
            product = lax.dot_general(
                left, ref["rmat"][...], (((1,), (1,)), ((), ())), preferred_element_type=f32
            )
            ref["tsend"][place] = (product * back).reshape(chunks, 8, lanes).astype(bf16)

        @pl.when(row == z)
        def _():
            for c in range(chunks):
                ref["trecv"][c, slot] = ref["tsend"][place, c]

        @pl.when(row != z)
        def _():
            for c in range(chunks):
                send(
                    ref["tsend"].at[place, c],
                    ref["trecv"].at[c, slot],
                    ref["t_ss"].at[0],
                    ref["t_rs"].at[c],
                    {"gx": row},
                )

    each(0, half, triangle)

    with jax.named_scope("sent"):
        await_bytes(ref["rhome"].at[pl.ds(0, nz - 1)], ref["r_ss"].at[0])
        await_bytes(ref["lhome"].at[pl.ds(0, half - 1)], ref["l_ss"].at[0])
        await_bytes(ref["peak_z"].at[pl.ds(0, nz - 1)], ref["pz_ss"].at[0])
        await_bytes(ref["peak_z"].at[pl.ds(0, nz - 1)], ref["pz_rs"].at[0])
    tops = jnp.max(ref["peak_z"][...], axis=0)
    ref["amax"][0:1, :] = tops[:, :64]
    ref["amax"][1:2, :] = tops[:, 64:]

    def over_x(c):
        with jax.named_scope("triwait"):
            await_bytes(ref["trecv"].at[c, pl.ds(0, half - 1)], ref["t_rs"].at[c])
        staged = ref["staged"]
        with jax.named_scope("relayt"):
            for s in range(8):
                for j in range(5):
                    staged[pl.ds(8 * j + s, 8, stride=40), :] = ref["trecv"][
                        c, s, :, 128 * j : 128 * j + 128
                    ].astype(f32)
            for g in range(5):
                parts = [staged[8 * (8 * g + p) : 8 * (8 * g + p) + 8, :] for p in range(8)]
                for b, part in enumerate(block_transpose(parts)):
                    ref["txsend"][c, b, :, 128 * g : 128 * g + 128] = part.astype(bf16)
            ref["tfull"][c, core, x] = ref["txsend"][c, x]
            for d in x_order:
                t = xp(d)
                send(
                    ref["txsend"].at[c, t],
                    ref["tfull"].at[c, core, x],
                    ref["tx_ss"].at[0],
                    ref["tx_rs"].at[c],
                    {"gy": t},
                )

    def over_core(c):
        with jax.named_scope("colwait"):
            await_bytes(ref["tfull"].at[c, core, pl.ds(0, nx - 1)], ref["tx_rs"].at[c])
        send(
            ref["tfull"].at[c, core],
            ref["tfull"].at[c, core],
            ref["d_ss"].at[0],
            ref["d_rs"].at[c],
            {"col": other},
        )

    out_gain = column(ref["out_gain"][...], 128)
    out_bias = column(ref["out_bias"][...], 128)

    def finish(c):
        with jax.named_scope("corewait"):
            await_bytes(ref["tfull"].at[c, other], ref["d_rs"].at[c])
        with jax.named_scope("finish"):
            values = ref["tfull"][c].astype(f32).reshape(128, lanes)
            average = jnp.mean(values, axis=0, keepdims=True)
            centred = values - average
            spread = jnp.mean(centred * centred, axis=0, keepdims=True)
            scaled = centred * lax.rsqrt(spread + epsilon)
            tnorm = jnp.concatenate(
                [scaled[:, 128 * k : 128 * k + 128] * out_gain + out_bias for k in range(5)], axis=1
            ).astype(bf16)
            mixing = jnp.dot(ref["out_w"][...], tnorm, preferred_element_type=f32)
            update = ref["gates"][c] * mixing
            for i in range(8):
                ref["held"][8 * c + i] = update[:, 80 * i : 80 * i + 80].astype(bf16)

    def store(c):
        block = pl.ds(8 * c, 8)
        return pltpu.make_async_copy(ref["held"].at[block], ref["out"].at[block], ref["out_sem"].at[c])

    for c in range(chunks):
        over_x(c)
    with jax.named_scope("sent2"):
        await_bytes(ref["tsend"].at[pl.ds(0, half - 1)], ref["t_ss"].at[0])
    for c in range(chunks + 1):
        if c < chunks:
            over_core(c)
        if c > 0:
            finish(c - 1)
            store(c - 1).start()
    await_bytes(ref["lhome"].at[pl.ds(0, nx - 1)], ref["tx_ss"].at[0])
    await_bytes(ref["lhome"], ref["d_ss"].at[0])
    for c in range(chunks):
        store(c).wait()


def solution(mesh):
    nz, nx = mesh.shape["gx"], mesh.shape["gy"]

    def on_device(
        pair_rep,
        pair_mask,
        amax_history,
        in_gain,
        in_bias,
        proj_weight,
        gate_weight,
        out_gain,
        out_bias,
        out_weight,
    ):
        _, ni, nj, width = pair_rep.shape
        held = proj_weight.shape[2]
        chunks = ni // 8
        lanes = 8 * nj
        half = nz // 2
        assert nx == 8 and nz == 16 and lanes == 640 and width == 128 and held == 64
        dma = pltpu.SemaphoreType.DMA
        operands = {
            "mask_h": pair_mask,
            "history_h": amax_history,
            "w_h": proj_weight.transpose(1, 2, 0),
            "gain_h": in_gain[None],
            "bias_h": in_bias[None],
            "gate_w_h": gate_weight.T,
            "out_gain_h": out_gain[None],
            "out_bias_h": out_bias[None],
            "out_w_h": out_weight.T,
            "pair_h": pair_rep,
        }
        scratch = {
            name[:-2]: pltpu.VMEM(value.shape, value.dtype)
            for name, value in operands.items()
            if name != "pair_h"
        }
        scratch.update(
            pair=pltpu.VMEM((ni, nj, width), bf16),
            held=pltpu.VMEM((ni, held, nj), bf16),
            out_sem=dma((chunks,)),
            in_sem=dma((len(operands) - 1,)),
            pair_sem=dma((chunks,)),
            normed=pltpu.VMEM((ni * nj, width), bf16),
            gates=pltpu.VMEM((chunks, held, lanes), f32),
            peakl=pltpu.VMEM((held, 128), f32),
            peakr=pltpu.VMEM((held, 128), f32),
            xsr=pltpu.VMEM((chunks, nx, 8, lanes), bf16),
            xsl=pltpu.VMEM((chunks, nx, 8, lanes), bf16),
            xrr=pltpu.VMEM((chunks, nx, 8, lanes), bf16),
            xrl=pltpu.VMEM((chunks, nx, 8, lanes), bf16),
            staged=pltpu.VMEM((8 * 40, 128), f32),
            readyr=pltpu.VMEM((8, chunks, 8, lanes), bf16),
            readyl=pltpu.VMEM((8, chunks, 8, lanes), bf16),
            rhome=pltpu.VMEM((nz, chunks, 8, lanes), bf16),
            rmat=pltpu.VMEM((lanes, lanes), bf16),
            lhome=pltpu.VMEM((half, chunks, 8, lanes), bf16),
            tsend=pltpu.VMEM((half, chunks, 8, lanes), bf16),
            trecv=pltpu.VMEM((chunks, half, 8, lanes), bf16),
            txsend=pltpu.VMEM((chunks, nx, 8, lanes), bf16),
            tfull=pltpu.VMEM((chunks, 2, nx, 8, lanes), bf16),
            peak_x=pltpu.VMEM((nx, 1, 128), f32),
            peak_z=pltpu.VMEM((nz, 1, 128), f32),
            known=pltpu.SemaphoreType.REGULAR((nz,)),
            px_ss=dma((1,)),
            px_rs=dma((1,)),
            pz_ss=dma((1,)),
            pz_rs=dma((1,)),
            xsr_ss=dma((1,)),
            xsr_rs=dma((chunks,)),
            xsl_ss=dma((1,)),
            xsl_rs=dma((chunks,)),
            r_ss=dma((1,)),
            r_rs=dma((nz,)),
            l_ss=dma((1,)),
            l_rs=dma((half,)),
            t_ss=dma((1,)),
            t_rs=dma((chunks,)),
            tx_ss=dma((1,)),
            tx_rs=dma((chunks,)),
            d_ss=dma((1,)),
            d_rs=dma((chunks,)),
        )
        names = (*operands, "out", "amax", *scratch)
        vmem = pl.BlockSpec(memory_space=pltpu.VMEM)
        update, amax = pl.pallas_call(
            functools.partial(kernel, (nz, nx, chunks, names)),
            out_shape=(
                jax.ShapeDtypeStruct((ni, held, nj), bf16),
                jax.ShapeDtypeStruct((2, held), f32),
            ),
            in_specs=[pl.BlockSpec(memory_space=pltpu.HBM)] * len(operands),
            out_specs=(pl.BlockSpec(memory_space=pltpu.HBM), vmem),
            scratch_shapes=list(scratch.values()),
            compiler_params=pltpu.CompilerParams(
                collective_id=0, has_side_effects=True, vmem_limit_bytes=67_043_328
            ),
            name="triangle",
        )(*operands.values())
        return update.transpose(0, 2, 1)[None], amax

    placed = (
        P("ga", "gx", "gy", None),
        P("ga", "gx", "gy"),
        P(None, "col"),
        P(),
        P(),
        P(None, None, "col"),
        P(None, "col"),
        P(),
        P(),
        P(None, "col"),
    )
    return jax.shard_map(
        on_device,
        mesh=mesh,
        in_specs=placed,
        out_specs=(P("ga", "gx", "gy", "col"), P("ga", "col")),
        check_vma=False,
    )
```

```python
import functools

import jax
import jax.numpy as jnp
from jax import lax
from jax.experimental import pallas as pl
from jax.experimental.pallas import tpu as pltpu
from jax.sharding import PartitionSpec as P

epsilon = 1e-05
format_limit = 448.0
MESH = pl.DeviceIdType.MESH
f32, bf16 = jnp.float32, jnp.bfloat16


def block_transpose(parts):
    parts = list(parts)
    shape = parts[0].shape
    block = lax.broadcasted_iota(jnp.int32, shape, len(shape) - 1) // 16
    for bit in (4, 2, 1):
        low = (block & bit) == 0
        for a in range(8):
            if a & bit:
                continue
            x, y = parts[a], parts[a | bit]
            parts[a] = jnp.where(low, x, pltpu.roll(y, 16 * bit, 1))
            parts[a | bit] = jnp.where(low, pltpu.roll(x, 128 - 16 * bit, 1), y)
    return parts


def kernel(sizes, *refs):
    nz, nx, chunks, names = sizes
    ref = dict(zip(names, refs))
    z, x, core = lax.axis_index("gx"), lax.axis_index("gy"), lax.axis_index("col")
    other = 1 - core
    half = nz // 2
    slot = lax.rem(z, half)
    lanes = 640

    def column(row, width):
        return jnp.broadcast_to(row, (width, row.shape[1])).T

    def load(name):
        return pltpu.make_async_copy(ref[name + "_h"], ref[name], ref["in_sem"].at[inputs.index(name)])

    inputs = [n[:-2] for n in names if n.endswith("_h") and n != "pair_h"]

    def pair_load(c):
        return pltpu.make_async_copy(
            ref["pair_h"].at[0, pl.ds(8 * c, 8)], ref["pair"].at[pl.ds(8 * c, 8)], ref["pair_sem"].at[c]
        )

    def send(src, dst, ss, rs, target):
        pltpu.make_async_remote_copy(
            src_ref=src, dst_ref=dst, send_sem=ss, recv_sem=rs, device_id=target, device_id_type=MESH
        ).start()

    def await_bytes(like, sem):
        pltpu.make_async_copy(like, like, sem).wait()

    def zp(d):
        return lax.rem(z + d, nz)

    def xp(d):
        return lax.rem(x + d, nx)

    rank = lax.rem(z + nz - 1, nz)

    def ranked(r):
        return lax.rem(r + 1, nz)

    def each(low, high, body):
        def step(i, carry):
            body(i)
            return carry

        lax.fori_loop(low, high, step, 0)

    barrier = pltpu.get_barrier_semaphore()
    for d in range(1, nx):
        pl.semaphore_signal(barrier, inc=1, device_id={"gy": xp(d)}, device_id_type=MESH)
    pl.semaphore_signal(barrier, inc=1, device_id={"col": other}, device_id_type=MESH)
    each(
        rank + 1,
        nz,
        lambda r: pl.semaphore_signal(
            barrier, inc=1, device_id={"gx": ranked(r)}, device_id_type=MESH
        ),
    )
    for name in inputs[:6]:
        load(name).start()
    for c in range(chunks):
        pair_load(c).start()
    for name in inputs[6:]:
        load(name).start()

    def enter():
        with jax.named_scope("entry"):
            pl.semaphore_wait(barrier, nx + rank)
        each(
            0,
            rank,
            lambda r: pl.semaphore_signal(
                ref["known"].at[z], inc=1, device_id={"gx": ranked(r)}, device_id_type=MESH
            ),
        )

    @pl.when(rank < nz - 1)
    def _():
        enter()

    with jax.named_scope("input"):
        for name in inputs:
            load(name).wait()

    x_order = []
    for d in range(nx // 2, 0, -1):
        x_order.append(d)
        if nx - d != d:
            x_order.append(nx - d)

    def x_send(kind, c):
        for d in x_order:
            t = xp(d)
            send(
                ref["xs" + kind].at[c, t],
                ref["xr" + kind].at[c, x],
                ref[f"xs{kind}_ss"].at[0],
                ref[f"xs{kind}_rs"].at[c],
                {"gy": t},
            )

    history = ref["history"][...]
    inverse = format_limit / history
    inverse_left = column(inverse[0:1, :], 128)
    inverse_right = column(inverse[1:2, :], 128)
    weights = ref["w"][...].reshape(256, 128)
    for c in range(chunks):
        with jax.named_scope("pair"):
            pair_load(c).wait()
        with jax.named_scope("norm"):
            rows = ref["pair"][8 * c : 8 * c + 8].reshape(lanes, 128).astype(f32)
            average = jnp.mean(rows, axis=-1, keepdims=True)
            centred = rows - average
            spread = jnp.mean(centred * centred, axis=-1, keepdims=True)
            flat = (
                centred * lax.rsqrt(spread + epsilon) * ref["gain"][...] + ref["bias"][...]
            ).astype(bf16)
            ref["normed"][lanes * c : lanes * c + lanes, :] = flat
            kept = ref["mask"][0, 8 * c : 8 * c + 8, :].astype(f32).T
            masked = jnp.concatenate(
                [flat[80 * i : 80 * i + 80] * kept[:, i : i + 1].astype(bf16) for i in range(8)], axis=0
            )
            proj = lax.dot_general(
                weights, masked, (((1,), (1,)), ((), ())), preferred_element_type=f32
            )
        with jax.named_scope("quant"):
            for kind, base, inv in (("r", 128, inverse_right), ("l", 0, inverse_left)):
                both = jax.nn.sigmoid(proj[base + 64 : base + 128]) * proj[base : base + 64]
                tiles = [both[:, 128 * k : 128 * k + 128] for k in range(5)]
                top = functools.reduce(jnp.maximum, [jnp.abs(tile) for tile in tiles])
                peak = ref["peak" + kind]
                peak[...] = top if c == 0 else jnp.maximum(peak[...], top)
                quant = jnp.concatenate(
                    [jnp.clip(tile * inv, -format_limit, format_limit) for tile in tiles], axis=1
                )
                ref["xs" + kind][c] = quant.astype(bf16).reshape(8, 8, lanes)
                ref["xr" + kind][c, x] = ref["xs" + kind][c, x]
                if kind == "r":
                    if c == 0:

                        @pl.when(rank == nz - 1)
                        def _():
                            enter()

                    x_send("r", c)
    for c in range(chunks):
        x_send("l", c)
    with jax.named_scope("peak"):
        tops = jnp.concatenate([ref["peakl"][...], ref["peakr"][...]], axis=0)
        ref["peak_x"][x] = jnp.max(tops.T, axis=0, keepdims=True)
        for d in x_order:
            send(
                ref["peak_x"].at[x],
                ref["peak_x"].at[x],
                ref["px_ss"].at[0],
                ref["px_rs"].at[0],
                {"gy": xp(d)},
            )
    with jax.named_scope("gate"):
        for c in range(chunks):
            ref["gates"][c] = jax.nn.sigmoid(
                lax.dot_general(
                    ref["gate_w"][...],
                    ref["normed"][lanes * c : lanes * c + lanes, :],
                    (((1,), (1,)), ((), ())),
                    preferred_element_type=f32,
                )
            )

    def gather_rows(kind, c):
        with jax.named_scope("xwait" + kind):
            await_bytes(ref["xr" + kind].at[c, pl.ds(0, nx - 1)], ref[f"xs{kind}_rs"].at[c])
        staged = ref["staged"]
        with jax.named_scope("relay" + kind):
            for g in range(5):
                parts = [
                    ref["xr" + kind][c, a, :, 128 * g : 128 * g + 128].astype(f32) for a in range(8)
                ]
                for p, part in enumerate(block_transpose(parts)):
                    staged[8 * (8 * g + p) : 8 * (8 * g + p) + 8, :] = part
            for s in range(8):
                tiles = [staged[pl.ds(8 * k + s, 8, stride=40), :] for k in range(5)]
                ref["ready" + kind][s, c] = jnp.concatenate(tiles, axis=1).astype(bf16)

    def send_right(c, t):
        send(
            ref["readyr"].at[lax.rem(t, half), c],
            ref["rhome"].at[z, c],
            ref["r_ss"].at[0],
            ref["r_rs"].at[z],
            {"gx": t},
        )

    def send_left(c, t):
        send(
            ref["readyl"].at[lax.rem(t, half), c],
            ref["lhome"].at[slot, c],
            ref["l_ss"].at[0],
            ref["l_rs"].at[0],
            {"gx": t},
        )

    def in_arc(t):
        e = lax.rem(t - z + nz, nz)
        return (e < half // 2) | (e > nz - half // 2) | (e == half // 2 + half * core)

    def send_peak(t):
        send(
            ref["peak_z"].at[z], ref["peak_z"].at[z], ref["pz_ss"].at[0], ref["pz_rs"].at[0], {"gx": t}
        )

    ahead = half - 2
    near = lax.min(rank + 1 + ahead, nz)

    def left_to(r):
        t = ranked(r)

        @pl.when(in_arc(t))
        def _():
            for c in range(chunks):
                send_left(c, t)

    def right_to(r):
        t = ranked(r)
        pl.semaphore_wait(ref["known"].at[t], 1)
        for c in range(chunks):
            send_right(c, t)

    def rest_to(r):
        right_to(r)
        left_to(r)
        send_peak(ranked(r))

    for c in range(chunks):
        gather_rows("r", c)
        ref["rhome"][z, c] = ref["readyr"][slot, c]
        each(0, rank, lambda r: send_right(c, ranked(r)))
    with jax.named_scope("near"):
        each(rank + 1, near, right_to)
    for c in range(chunks):
        gather_rows("l", c)
        ref["lhome"][slot, c] = ref["readyl"][slot, c]

        def left_below(r):
            t = ranked(r)

            @pl.when(in_arc(t))
            def _():
                send_left(c, t)

        each(0, rank, left_below)
    each(rank + 1, near, left_to)
    with jax.named_scope("peakwait"):
        await_bytes(ref["peak_x"].at[pl.ds(0, nx - 1)], ref["px_rs"].at[0])
    ref["peak_z"][z] = jnp.max(ref["peak_x"][...], axis=0)
    each(0, rank, lambda r: send_peak(ranked(r)))
    each(rank + 1, near, lambda r: send_peak(ranked(r)))
    with jax.named_scope("higher"):
        each(near, nz, rest_to)
    with jax.named_scope("sentx"):
        await_bytes(ref["peak_x"].at[pl.ds(0, nx - 1)], ref["px_ss"].at[0])
        await_bytes(ref["lhome"].at[pl.ds(0, nx - 1)], ref["xsr_ss"].at[0])
        await_bytes(ref["lhome"].at[pl.ds(0, nx - 1)], ref["xsl_ss"].at[0])

    def right_arrived(n):
        source = zp(n)
        await_bytes(ref["rhome"].at[source], ref["r_rs"].at[source])

    with jax.named_scope("rightwait"):
        each(1, nz, right_arrived)
    with jax.named_scope("rmat"):
        for t in range(5):
            granules = []
            for b in range(8):
                for g in (2 * t, 2 * t + 1):
                    granules.append(ref["rhome"][2 * b + g // 5, g % 5].astype(f32))
            ref["rmat"][128 * t : 128 * t + 128, :] = jnp.concatenate(granules, axis=0).astype(bf16)

    product_scale = history[0:1, :] * history[1:2, :] * (1.0 / format_limit / format_limit)
    channel = 8 * x + slot
    here = lax.broadcasted_iota(jnp.int32, product_scale.shape, 1) == channel
    back = jnp.sum(jnp.where(here, product_scale, 0.0), axis=1, keepdims=True)
    first = z - half // 2 + core + nz
    with jax.named_scope("leftwait"):
        await_bytes(ref["lhome"].at[pl.ds(0, half - 1)], ref["l_rs"].at[0])

    for c in range(chunks):
        with jax.named_scope("dot"):
            left = jnp.concatenate(
                [ref["lhome"][place, c].astype(f32) for place in range(half)], axis=0
            ).astype(bf16)
            product = lax.dot_general(
                left, ref["rmat"][...], (((1,), (1,)), ((), ())), preferred_element_type=f32
            )
            ref["tsend"][c] = (product * back).reshape(half, 8, lanes).astype(bf16)
        ref["trecv"][c, slot] = ref["tsend"][c, slot]

        def triangle(n):
            place = lax.rem(slot + n, half)
            row = lax.rem(first + lax.rem(place - lax.rem(first, half) + half, half), nz)
            send(
                ref["tsend"].at[c, place],
                ref["trecv"].at[c, slot],
                ref["t_ss"].at[0],
                ref["t_rs"].at[c],
                {"gx": row},
            )

        each(1, half, triangle)

    with jax.named_scope("sent"):
        await_bytes(ref["rhome"].at[pl.ds(0, nz - 1)], ref["r_ss"].at[0])
        await_bytes(ref["lhome"].at[pl.ds(0, half - 1)], ref["l_ss"].at[0])
        await_bytes(ref["peak_z"].at[pl.ds(0, nz - 1)], ref["pz_ss"].at[0])
        await_bytes(ref["peak_z"].at[pl.ds(0, nz - 1)], ref["pz_rs"].at[0])
    tops = jnp.max(ref["peak_z"][...], axis=0)
    ref["amax"][0:1, :] = tops[:, :64]
    ref["amax"][1:2, :] = tops[:, 64:]

    def over_x(c):
        with jax.named_scope("triwait"):
            await_bytes(ref["trecv"].at[c, pl.ds(0, half - 1)], ref["t_rs"].at[c])
        staged = ref["staged"]
        with jax.named_scope("relayt"):
            for s in range(8):
                for j in range(5):
                    staged[pl.ds(8 * j + s, 8, stride=40), :] = ref["trecv"][
                        c, s, :, 128 * j : 128 * j + 128
                    ].astype(f32)
            for g in range(5):
                parts = [staged[8 * (8 * g + p) : 8 * (8 * g + p) + 8, :] for p in range(8)]
                for b, part in enumerate(block_transpose(parts)):
                    ref["txsend"][c, b, :, 128 * g : 128 * g + 128] = part.astype(bf16)
            ref["tfull"][c, core, x] = ref["txsend"][c, x]
            for d in x_order:
                t = xp(d)
                send(
                    ref["txsend"].at[c, t],
                    ref["tfull"].at[c, core, x],
                    ref["tx_ss"].at[0],
                    ref["tx_rs"].at[c],
                    {"gy": t},
                )

    def over_core(c):
        with jax.named_scope("colwait"):
            await_bytes(ref["tfull"].at[c, core, pl.ds(0, nx - 1)], ref["tx_rs"].at[c])
        send(
            ref["tfull"].at[c, core],
            ref["tfull"].at[c, core],
            ref["d_ss"].at[0],
            ref["d_rs"].at[c],
            {"col": other},
        )

    out_gain = column(ref["out_gain"][...], 128)
    out_bias = column(ref["out_bias"][...], 128)

    def finish(c):
        with jax.named_scope("corewait"):
            await_bytes(ref["tfull"].at[c, other], ref["d_rs"].at[c])
        with jax.named_scope("finish"):
            values = ref["tfull"][c].astype(f32).reshape(128, lanes)
            average = jnp.mean(values, axis=0, keepdims=True)
            centred = values - average
            spread = jnp.mean(centred * centred, axis=0, keepdims=True)
            scaled = centred * lax.rsqrt(spread + epsilon)
            tnorm = jnp.concatenate(
                [scaled[:, 128 * k : 128 * k + 128] * out_gain + out_bias for k in range(5)], axis=1
            ).astype(bf16)
            mixing = jnp.dot(ref["out_w"][...], tnorm, preferred_element_type=f32)
            update = ref["gates"][c] * mixing
            for i in range(8):
                ref["held"][8 * c + i] = update[:, 80 * i : 80 * i + 80].astype(bf16)

    def store(c):
        block = pl.ds(8 * c, 8)
        return pltpu.make_async_copy(ref["held"].at[block], ref["out"].at[block], ref["out_sem"].at[c])

    for c in range(chunks):
        over_x(c)
    with jax.named_scope("sent2"):
        await_bytes(ref["lhome"].at[pl.ds(0, half - 1)], ref["t_ss"].at[0])
    for c in range(chunks + 1):
        if c < chunks:
            over_core(c)
        if c > 0:
            finish(c - 1)
            store(c - 1).start()
    await_bytes(ref["lhome"].at[pl.ds(0, nx - 1)], ref["tx_ss"].at[0])
    await_bytes(ref["lhome"], ref["d_ss"].at[0])
    for c in range(chunks):
        store(c).wait()


def solution(mesh):
    nz, nx = mesh.shape["gx"], mesh.shape["gy"]

    def on_device(
        pair_rep,
        pair_mask,
        amax_history,
        in_gain,
        in_bias,
        proj_weight,
        gate_weight,
        out_gain,
        out_bias,
        out_weight,
    ):
        _, ni, nj, width = pair_rep.shape
        held = proj_weight.shape[2]
        chunks = ni // 8
        lanes = 8 * nj
        half = nz // 2
        assert nx == 8 and nz == 16 and lanes == 640 and width == 128 and held == 64
        dma = pltpu.SemaphoreType.DMA
        operands = {
            "mask_h": pair_mask,
            "history_h": amax_history,
            "w_h": proj_weight.transpose(1, 2, 0),
            "gain_h": in_gain[None],
            "bias_h": in_bias[None],
            "gate_w_h": gate_weight.T,
            "out_gain_h": out_gain[None],
            "out_bias_h": out_bias[None],
            "out_w_h": out_weight.T,
            "pair_h": pair_rep,
        }
        scratch = {
            name[:-2]: pltpu.VMEM(value.shape, value.dtype)
            for name, value in operands.items()
            if name != "pair_h"
        }
        scratch.update(
            pair=pltpu.VMEM((ni, nj, width), bf16),
            held=pltpu.VMEM((ni, held, nj), bf16),
            out_sem=dma((chunks,)),
            in_sem=dma((len(operands) - 1,)),
            pair_sem=dma((chunks,)),
            normed=pltpu.VMEM((ni * nj, width), bf16),
            gates=pltpu.VMEM((chunks, held, lanes), f32),
            peakl=pltpu.VMEM((held, 128), f32),
            peakr=pltpu.VMEM((held, 128), f32),
            xsr=pltpu.VMEM((chunks, nx, 8, lanes), bf16),
            xsl=pltpu.VMEM((chunks, nx, 8, lanes), bf16),
            xrr=pltpu.VMEM((chunks, nx, 8, lanes), bf16),
            xrl=pltpu.VMEM((chunks, nx, 8, lanes), bf16),
            staged=pltpu.VMEM((8 * 40, 128), f32),
            readyr=pltpu.VMEM((8, chunks, 8, lanes), bf16),
            readyl=pltpu.VMEM((8, chunks, 8, lanes), bf16),
            rhome=pltpu.VMEM((nz, chunks, 8, lanes), bf16),
            rmat=pltpu.VMEM((lanes, lanes), bf16),
            lhome=pltpu.VMEM((half, chunks, 8, lanes), bf16),
            tsend=pltpu.VMEM((chunks, half, 8, lanes), bf16),
            trecv=pltpu.VMEM((chunks, half, 8, lanes), bf16),
            txsend=pltpu.VMEM((chunks, nx, 8, lanes), bf16),
            tfull=pltpu.VMEM((chunks, 2, nx, 8, lanes), bf16),
            peak_x=pltpu.VMEM((nx, 1, 128), f32),
            peak_z=pltpu.VMEM((nz, 1, 128), f32),
            known=pltpu.SemaphoreType.REGULAR((nz,)),
            px_ss=dma((1,)),
            px_rs=dma((1,)),
            pz_ss=dma((1,)),
            pz_rs=dma((1,)),
            xsr_ss=dma((1,)),
            xsr_rs=dma((chunks,)),
            xsl_ss=dma((1,)),
            xsl_rs=dma((chunks,)),
            r_ss=dma((1,)),
            r_rs=dma((nz,)),
            l_ss=dma((1,)),
            l_rs=dma((1,)),
            t_ss=dma((1,)),
            t_rs=dma((chunks,)),
            tx_ss=dma((1,)),
            tx_rs=dma((chunks,)),
            d_ss=dma((1,)),
            d_rs=dma((chunks,)),
        )
        names = (*operands, "out", "amax", *scratch)
        vmem = pl.BlockSpec(memory_space=pltpu.VMEM)
        update, amax = pl.pallas_call(
            functools.partial(kernel, (nz, nx, chunks, names)),
            out_shape=(
                jax.ShapeDtypeStruct((ni, held, nj), bf16),
                jax.ShapeDtypeStruct((2, held), f32),
            ),
            in_specs=[pl.BlockSpec(memory_space=pltpu.HBM)] * len(operands),
            out_specs=(pl.BlockSpec(memory_space=pltpu.HBM), vmem),
            scratch_shapes=list(scratch.values()),
            compiler_params=pltpu.CompilerParams(
                collective_id=0, has_side_effects=True, vmem_limit_bytes=67_043_328
            ),
            name="triangle",
        )(*operands.values())
        return update.transpose(0, 2, 1)[None], amax

    placed = (
        P("ga", "gx", "gy", None),
        P("ga", "gx", "gy"),
        P(None, "col"),
        P(),
        P(),
        P(None, None, "col"),
        P(None, "col"),
        P(),
        P(),
        P(None, "col"),
    )
    return jax.shard_map(
        on_device,
        mesh=mesh,
        in_specs=placed,
        out_specs=(P("ga", "gx", "gy", "col"), P("ga", "col")),
        check_vma=False,
    )
```

```python
import functools

import jax
import jax.numpy as jnp
from jax import lax
from jax.experimental import pallas as pl
from jax.experimental.pallas import tpu as pltpu
from jax.sharding import PartitionSpec as P

epsilon = 1e-05
format_limit = 448.0
MESH = pl.DeviceIdType.MESH
f32, bf16 = jnp.float32, jnp.bfloat16


def block_transpose(parts):
    parts = list(parts)
    shape = parts[0].shape
    block = lax.broadcasted_iota(jnp.int32, shape, len(shape) - 1) // 16
    for bit in (4, 2, 1):
        low = (block & bit) == 0
        for a in range(8):
            if a & bit:
                continue
            x, y = parts[a], parts[a | bit]
            parts[a] = jnp.where(low, x, pltpu.roll(y, 16 * bit, 1))
            parts[a | bit] = jnp.where(low, pltpu.roll(x, 128 - 16 * bit, 1), y)
    return parts


def kernel(sizes, *refs):
    nz, nx, chunks, names = sizes
    ref = dict(zip(names, refs))
    z, x, core = lax.axis_index("gx"), lax.axis_index("gy"), lax.axis_index("col")
    other = 1 - core
    half = nz // 2
    slot = lax.rem(z, half)
    lanes = 640

    def column(row, width):
        return jnp.broadcast_to(row, (width, row.shape[1])).T

    def load(name):
        return pltpu.make_async_copy(ref[name + "_h"], ref[name], ref["in_sem"].at[inputs.index(name)])

    inputs = [n[:-2] for n in names if n.endswith("_h") and n != "pair_h"]

    def pair_load(c):
        return pltpu.make_async_copy(
            ref["pair_h"].at[0, pl.ds(8 * c, 8)], ref["pair"].at[pl.ds(8 * c, 8)], ref["pair_sem"].at[c]
        )

    def send(src, dst, ss, rs, target):
        pltpu.make_async_remote_copy(
            src_ref=src, dst_ref=dst, send_sem=ss, recv_sem=rs, device_id=target, device_id_type=MESH
        ).start()

    def await_bytes(like, sem):
        pltpu.make_async_copy(like, like, sem).wait()

    def zp(d):
        return lax.rem(z + d, nz)

    def xp(d):
        return lax.rem(x + d, nx)

    rank = lax.rem(z + nz - 1, nz)

    def ranked(r):
        return lax.rem(r + 1, nz)

    def each(low, high, body):
        def step(i, carry):
            body(i)
            return carry

        lax.fori_loop(low, high, step, 0)

    barrier = pltpu.get_barrier_semaphore()
    for d in range(1, nx):
        pl.semaphore_signal(barrier, inc=1, device_id={"gy": xp(d)}, device_id_type=MESH)
    pl.semaphore_signal(barrier, inc=1, device_id={"col": other}, device_id_type=MESH)
    each(
        rank + 1,
        nz,
        lambda r: pl.semaphore_signal(
            barrier, inc=1, device_id={"gx": ranked(r)}, device_id_type=MESH
        ),
    )
    for name in inputs[:6]:
        load(name).start()
    for c in range(chunks):
        pair_load(c).start()
    for name in inputs[6:]:
        load(name).start()

    def enter():
        with jax.named_scope("entry"):
            pl.semaphore_wait(barrier, nx + rank)
        each(
            0,
            rank,
            lambda r: pl.semaphore_signal(
                ref["known"].at[z], inc=1, device_id={"gx": ranked(r)}, device_id_type=MESH
            ),
        )

    @pl.when(rank < nz - 1)
    def _():
        enter()

    with jax.named_scope("input"):
        for name in inputs:
            load(name).wait()

    x_order = []
    for d in range(nx // 2, 0, -1):
        x_order.append(d)
        if nx - d != d:
            x_order.append(nx - d)

    def x_send(kind, c):
        for d in x_order:
            t = xp(d)
            send(
                ref["xs" + kind].at[c, t],
                ref["xr" + kind].at[c, x],
                ref[f"xs{kind}_ss"].at[0],
                ref[f"xs{kind}_rs"].at[c],
                {"gy": t},
            )

    history = ref["history"][...]
    inverse = format_limit / history
    inverse_left = column(inverse[0:1, :], 128)
    inverse_right = column(inverse[1:2, :], 128)
    weights = ref["w"][...].reshape(256, 128)
    for c in range(chunks):
        with jax.named_scope("pair"):
            pair_load(c).wait()
        with jax.named_scope("norm"):
            rows = ref["pair"][8 * c : 8 * c + 8].reshape(lanes, 128).astype(f32)
            average = jnp.mean(rows, axis=-1, keepdims=True)
            centred = rows - average
            spread = jnp.mean(centred * centred, axis=-1, keepdims=True)
            flat = (
                centred * lax.rsqrt(spread + epsilon) * ref["gain"][...] + ref["bias"][...]
            ).astype(bf16)
            ref["normed"][lanes * c : lanes * c + lanes, :] = flat
            kept = ref["mask"][0, 8 * c : 8 * c + 8, :].astype(f32).T
            masked = jnp.concatenate(
                [flat[80 * i : 80 * i + 80] * kept[:, i : i + 1].astype(bf16) for i in range(8)], axis=0
            )
            proj = lax.dot_general(
                weights, masked, (((1,), (1,)), ((), ())), preferred_element_type=f32
            )
        with jax.named_scope("quant"):
            for kind, base, inv in (("r", 128, inverse_right), ("l", 0, inverse_left)):
                both = jax.nn.sigmoid(proj[base + 64 : base + 128]) * proj[base : base + 64]
                tiles = [both[:, 128 * k : 128 * k + 128] for k in range(5)]
                top = functools.reduce(jnp.maximum, [jnp.abs(tile) for tile in tiles])
                peak = ref["peak" + kind]
                peak[...] = top if c == 0 else jnp.maximum(peak[...], top)
                quant = jnp.concatenate(
                    [jnp.clip(tile * inv, -format_limit, format_limit) for tile in tiles], axis=1
                )
                ref["xs" + kind][c] = quant.astype(bf16).reshape(8, 8, lanes)
                ref["xr" + kind][c, x] = ref["xs" + kind][c, x]
                if kind == "r":
                    if c == 0:

                        @pl.when(rank == nz - 1)
                        def _():
                            enter()

                    x_send("r", c)
    for c in range(chunks):
        x_send("l", c)
    with jax.named_scope("peak"):
        tops = jnp.concatenate([ref["peakl"][...], ref["peakr"][...]], axis=0)
        ref["peak_x"][x] = jnp.max(tops.T, axis=0, keepdims=True)
        for d in x_order:
            send(
                ref["peak_x"].at[x],
                ref["peak_x"].at[x],
                ref["px_ss"].at[0],
                ref["px_rs"].at[0],
                {"gy": xp(d)},
            )
    with jax.named_scope("gate"):
        for c in range(chunks):
            ref["gates"][c] = jax.nn.sigmoid(
                lax.dot_general(
                    ref["gate_w"][...],
                    ref["normed"][lanes * c : lanes * c + lanes, :],
                    (((1,), (1,)), ((), ())),
                    preferred_element_type=f32,
                )
            )

    def gather_rows(kind, c):
        with jax.named_scope("xwait" + kind):
            await_bytes(ref["xr" + kind].at[c, pl.ds(0, nx - 1)], ref[f"xs{kind}_rs"].at[c])
        staged = ref["staged"]
        with jax.named_scope("relay" + kind):
            for g in range(5):
                parts = [
                    ref["xr" + kind][c, a, :, 128 * g : 128 * g + 128].astype(f32) for a in range(8)
                ]
                for p, part in enumerate(block_transpose(parts)):
                    staged[8 * (8 * g + p) : 8 * (8 * g + p) + 8, :] = part
            for s in range(8):
                tiles = [staged[pl.ds(8 * k + s, 8, stride=40), :] for k in range(5)]
                ref["ready" + kind][s, c] = jnp.concatenate(tiles, axis=1).astype(bf16)

    def send_right(c, t):
        send(
            ref["readyr"].at[lax.rem(t, half), c],
            ref["rhome"].at[z, c],
            ref["r_ss"].at[0],
            ref["r_rs"].at[z],
            {"gx": t},
        )

    def send_left(c, t):
        send(
            ref["readyl"].at[lax.rem(t, half), c],
            ref["lhome"].at[slot, c],
            ref["l_ss"].at[0],
            ref["l_rs"].at[0],
            {"gx": t},
        )

    def in_arc(t):
        e = lax.rem(t - z + nz, nz)
        return (e < half // 2) | (e > nz - half // 2) | (e == half // 2 + half * core)

    def send_peak(t):
        send(
            ref["peak_z"].at[z], ref["peak_z"].at[z], ref["pz_ss"].at[0], ref["pz_rs"].at[0], {"gx": t}
        )

    ahead = half - 2
    near = lax.min(rank + 1 + ahead, nz)
    soon = lax.min(rank + 3, nz)

    def known_to(r):
        pl.semaphore_wait(ref["known"].at[ranked(r)], 1)


    def left_to(r):
        t = ranked(r)

        @pl.when(in_arc(t))
        def _():
            for c in range(chunks):
                send_left(c, t)

    def right_to(r):
        t = ranked(r)
        pl.semaphore_wait(ref["known"].at[t], 1)
        for c in range(chunks):
            send_right(c, t)

    def rest_to(r):
        right_to(r)
        left_to(r)
        send_peak(ranked(r))

    for c in range(chunks):
        gather_rows("r", c)
        ref["rhome"][z, c] = ref["readyr"][slot, c]
        if c == 1:
            each(rank + 1, soon, known_to)
        if c >= 1:
            for b in (0, 1) if c == 1 else (c,):
                each(rank + 1, soon, lambda r: send_right(b, ranked(r)))
        each(0, rank, lambda r: send_right(c, ranked(r)))
    with jax.named_scope("near"):
        each(soon, near, right_to)
    for c in range(chunks):
        gather_rows("l", c)
        ref["lhome"][slot, c] = ref["readyl"][slot, c]

        def left_below(r):
            t = ranked(r)

            @pl.when(in_arc(t))
            def _():
                send_left(c, t)

        each(0, rank, left_below)
    each(rank + 1, near, left_to)
    with jax.named_scope("peakwait"):
        await_bytes(ref["peak_x"].at[pl.ds(0, nx - 1)], ref["px_rs"].at[0])
    ref["peak_z"][z] = jnp.max(ref["peak_x"][...], axis=0)
    each(0, rank, lambda r: send_peak(ranked(r)))
    each(rank + 1, near, lambda r: send_peak(ranked(r)))
    with jax.named_scope("higher"):
        each(near, nz, rest_to)
    with jax.named_scope("sentx"):
        await_bytes(ref["peak_x"].at[pl.ds(0, nx - 1)], ref["px_ss"].at[0])
        await_bytes(ref["lhome"].at[pl.ds(0, nx - 1)], ref["xsr_ss"].at[0])
        await_bytes(ref["lhome"].at[pl.ds(0, nx - 1)], ref["xsl_ss"].at[0])

    def right_arrived(n):
        source = zp(n)
        await_bytes(ref["rhome"].at[source], ref["r_rs"].at[source])

    with jax.named_scope("rightwait"):
        each(1, nz, right_arrived)
    with jax.named_scope("rmat"):
        for t in range(5):
            granules = []
            for b in range(8):
                for g in (2 * t, 2 * t + 1):
                    granules.append(ref["rhome"][2 * b + g // 5, g % 5].astype(f32))
            ref["rmat"][128 * t : 128 * t + 128, :] = jnp.concatenate(granules, axis=0).astype(bf16)

    product_scale = history[0:1, :] * history[1:2, :] * (1.0 / format_limit / format_limit)
    channel = 8 * x + slot
    here = lax.broadcasted_iota(jnp.int32, product_scale.shape, 1) == channel
    back = jnp.sum(jnp.where(here, product_scale, 0.0), axis=1, keepdims=True)
    first = z - half // 2 + core + nz
    with jax.named_scope("leftwait"):
        await_bytes(ref["lhome"].at[pl.ds(0, half - 1)], ref["l_rs"].at[0])

    for c in range(chunks):
        with jax.named_scope("dot"):
            left = jnp.concatenate(
                [ref["lhome"][place, c].astype(f32) for place in range(half)], axis=0
            ).astype(bf16)
            product = lax.dot_general(
                left, ref["rmat"][...], (((1,), (1,)), ((), ())), preferred_element_type=f32
            )
            ref["tsend"][c] = (product * back).reshape(half, 8, lanes).astype(bf16)
        ref["trecv"][c, slot] = ref["tsend"][c, slot]

        def triangle(n):
            place = lax.rem(slot + n, half)
            row = lax.rem(first + lax.rem(place - lax.rem(first, half) + half, half), nz)
            send(
                ref["tsend"].at[c, place],
                ref["trecv"].at[c, slot],
                ref["t_ss"].at[0],
                ref["t_rs"].at[c],
                {"gx": row},
            )

        each(1, half, triangle)

    with jax.named_scope("sent"):
        await_bytes(ref["rhome"].at[pl.ds(0, nz - 1)], ref["r_ss"].at[0])
        await_bytes(ref["lhome"].at[pl.ds(0, half - 1)], ref["l_ss"].at[0])
        await_bytes(ref["peak_z"].at[pl.ds(0, nz - 1)], ref["pz_ss"].at[0])
        await_bytes(ref["peak_z"].at[pl.ds(0, nz - 1)], ref["pz_rs"].at[0])
    tops = jnp.max(ref["peak_z"][...], axis=0)
    ref["amax"][0:1, :] = tops[:, :64]
    ref["amax"][1:2, :] = tops[:, 64:]

    def over_x(c):
        with jax.named_scope("triwait"):
            await_bytes(ref["trecv"].at[c, pl.ds(0, half - 1)], ref["t_rs"].at[c])
        staged = ref["staged"]
        with jax.named_scope("relayt"):
            for s in range(8):
                for j in range(5):
                    staged[pl.ds(8 * j + s, 8, stride=40), :] = ref["trecv"][
                        c, s, :, 128 * j : 128 * j + 128
                    ].astype(f32)
            for g in range(5):
                parts = [staged[8 * (8 * g + p) : 8 * (8 * g + p) + 8, :] for p in range(8)]
                for b, part in enumerate(block_transpose(parts)):
                    ref["txsend"][c, b, :, 128 * g : 128 * g + 128] = part.astype(bf16)
            ref["tfull"][c, core, x] = ref["txsend"][c, x]
            for d in x_order:
                t = xp(d)
                send(
                    ref["txsend"].at[c, t],
                    ref["tfull"].at[c, core, x],
                    ref["tx_ss"].at[0],
                    ref["tx_rs"].at[c],
                    {"gy": t},
                )

    def over_core(c):
        with jax.named_scope("colwait"):
            await_bytes(ref["tfull"].at[c, core, pl.ds(0, nx - 1)], ref["tx_rs"].at[c])
        send(
            ref["tfull"].at[c, core],
            ref["tfull"].at[c, core],
            ref["d_ss"].at[0],
            ref["d_rs"].at[c],
            {"col": other},
        )

    out_gain = column(ref["out_gain"][...], 128)
    out_bias = column(ref["out_bias"][...], 128)

    def finish(c):
        with jax.named_scope("corewait"):
            await_bytes(ref["tfull"].at[c, other], ref["d_rs"].at[c])
        with jax.named_scope("finish"):
            values = ref["tfull"][c].astype(f32).reshape(128, lanes)
            average = jnp.mean(values, axis=0, keepdims=True)
            centred = values - average
            spread = jnp.mean(centred * centred, axis=0, keepdims=True)
            scaled = centred * lax.rsqrt(spread + epsilon)
            tnorm = jnp.concatenate(
                [scaled[:, 128 * k : 128 * k + 128] * out_gain + out_bias for k in range(5)], axis=1
            ).astype(bf16)
            mixing = jnp.dot(ref["out_w"][...], tnorm, preferred_element_type=f32)
            update = ref["gates"][c] * mixing
            for i in range(8):
                ref["held"][8 * c + i] = update[:, 80 * i : 80 * i + 80].astype(bf16)

    def store(c):
        block = pl.ds(8 * c, 8)
        return pltpu.make_async_copy(ref["held"].at[block], ref["out"].at[block], ref["out_sem"].at[c])

    for c in range(chunks):
        over_x(c)
    with jax.named_scope("sent2"):
        await_bytes(ref["lhome"].at[pl.ds(0, half - 1)], ref["t_ss"].at[0])
    for c in range(chunks + 1):
        if c < chunks:
            over_core(c)
        if c > 0:
            finish(c - 1)
            store(c - 1).start()
    await_bytes(ref["lhome"].at[pl.ds(0, nx - 1)], ref["tx_ss"].at[0])
    await_bytes(ref["lhome"], ref["d_ss"].at[0])
    for c in range(chunks):
        store(c).wait()


def solution(mesh):
    nz, nx = mesh.shape["gx"], mesh.shape["gy"]

    def on_device(
        pair_rep,
        pair_mask,
        amax_history,
        in_gain,
        in_bias,
        proj_weight,
        gate_weight,
        out_gain,
        out_bias,
        out_weight,
    ):
        _, ni, nj, width = pair_rep.shape
        held = proj_weight.shape[2]
        chunks = ni // 8
        lanes = 8 * nj
        half = nz // 2
        assert nx == 8 and nz == 16 and lanes == 640 and width == 128 and held == 64
        dma = pltpu.SemaphoreType.DMA
        operands = {
            "mask_h": pair_mask,
            "history_h": amax_history,
            "w_h": proj_weight.transpose(1, 2, 0),
            "gain_h": in_gain[None],
            "bias_h": in_bias[None],
            "gate_w_h": gate_weight.T,
            "out_gain_h": out_gain[None],
            "out_bias_h": out_bias[None],
            "out_w_h": out_weight.T,
            "pair_h": pair_rep,
        }
        scratch = {
            name[:-2]: pltpu.VMEM(value.shape, value.dtype)
            for name, value in operands.items()
            if name != "pair_h"
        }
        scratch.update(
            pair=pltpu.VMEM((ni, nj, width), bf16),
            held=pltpu.VMEM((ni, held, nj), bf16),
            out_sem=dma((chunks,)),
            in_sem=dma((len(operands) - 1,)),
            pair_sem=dma((chunks,)),
            normed=pltpu.VMEM((ni * nj, width), bf16),
            gates=pltpu.VMEM((chunks, held, lanes), f32),
            peakl=pltpu.VMEM((held, 128), f32),
            peakr=pltpu.VMEM((held, 128), f32),
            xsr=pltpu.VMEM((chunks, nx, 8, lanes), bf16),
            xsl=pltpu.VMEM((chunks, nx, 8, lanes), bf16),
            xrr=pltpu.VMEM((chunks, nx, 8, lanes), bf16),
            xrl=pltpu.VMEM((chunks, nx, 8, lanes), bf16),
            staged=pltpu.VMEM((8 * 40, 128), f32),
            readyr=pltpu.VMEM((8, chunks, 8, lanes), bf16),
            readyl=pltpu.VMEM((8, chunks, 8, lanes), bf16),
            rhome=pltpu.VMEM((nz, chunks, 8, lanes), bf16),
            rmat=pltpu.VMEM((lanes, lanes), bf16),
            lhome=pltpu.VMEM((half, chunks, 8, lanes), bf16),
            tsend=pltpu.VMEM((chunks, half, 8, lanes), bf16),
            trecv=pltpu.VMEM((chunks, half, 8, lanes), bf16),
            txsend=pltpu.VMEM((chunks, nx, 8, lanes), bf16),
            tfull=pltpu.VMEM((chunks, 2, nx, 8, lanes), bf16),
            peak_x=pltpu.VMEM((nx, 1, 128), f32),
            peak_z=pltpu.VMEM((nz, 1, 128), f32),
            known=pltpu.SemaphoreType.REGULAR((nz,)),
            px_ss=dma((1,)),
            px_rs=dma((1,)),
            pz_ss=dma((1,)),
            pz_rs=dma((1,)),
            xsr_ss=dma((1,)),
            xsr_rs=dma((chunks,)),
            xsl_ss=dma((1,)),
            xsl_rs=dma((chunks,)),
            r_ss=dma((1,)),
            r_rs=dma((nz,)),
            l_ss=dma((1,)),
            l_rs=dma((1,)),
            t_ss=dma((1,)),
            t_rs=dma((chunks,)),
            tx_ss=dma((1,)),
            tx_rs=dma((chunks,)),
            d_ss=dma((1,)),
            d_rs=dma((chunks,)),
        )
        names = (*operands, "out", "amax", *scratch)
        vmem = pl.BlockSpec(memory_space=pltpu.VMEM)
        update, amax = pl.pallas_call(
            functools.partial(kernel, (nz, nx, chunks, names)),
            out_shape=(
                jax.ShapeDtypeStruct((ni, held, nj), bf16),
                jax.ShapeDtypeStruct((2, held), f32),
            ),
            in_specs=[pl.BlockSpec(memory_space=pltpu.HBM)] * len(operands),
            out_specs=(pl.BlockSpec(memory_space=pltpu.HBM), vmem),
            scratch_shapes=list(scratch.values()),
            compiler_params=pltpu.CompilerParams(
                collective_id=0, has_side_effects=True, vmem_limit_bytes=67_043_328
            ),
            name="triangle",
        )(*operands.values())
        return update.transpose(0, 2, 1)[None], amax

    placed = (
        P("ga", "gx", "gy", None),
        P("ga", "gx", "gy"),
        P(None, "col"),
        P(),
        P(),
        P(None, None, "col"),
        P(None, "col"),
        P(),
        P(),
        P(None, "col"),
    )
    return jax.shard_map(
        on_device,
        mesh=mesh,
        in_specs=placed,
        out_specs=(P("ga", "gx", "gy", "col"), P("ga", "col")),
        check_vma=False,
    )
```
